32 devices in a mesh: trial: 2 (over core), qa: 4 (over y, x), qb: 4 (over z).
Axes of the slice: x: 2, y: 2, z: 4, core: 2. Of those that a mesh axis runs over, the one named last changes fastest.
Arguments:
- wave_parts: float32 [4, 64, 128, 128], P('trial', ('qa', 'qb')), parts along dimension 0, may hold values from -6 to 6
- level_table: float32 [128, 128, 128], P(('trial', 'qa', 'qb')), parts along dimension 0, may hold values from -2 to 2
- diagonal_angles: float32 [6, 128], P('trial'), parts along dimension 0, may hold values from 0.3 to 1.2
- turn_angles: float32 [6, 4], P('trial'), parts along dimension 0, may hold values from 0.3 to 1.2
Outputs:
- final_parts: float32 [4, 64, 128, 128], P('trial', ('qa', 'qb')), parts along dimension 0
The draws below stay inside these ranges and needn't reach their ends.
There are 2 independent parts, one for each index of `trial`. The reference program is written for one: setup_inputs(seed, part) draws one part's arguments, and reference() takes and returns one part's arrays. A program takes and returns all parts, laid end to end along the dimension named above; each array names one. Nothing has to cross between parts.
All inputs are finite; a program needn't handle non-finite values.
Results may differ from the reference program's by a relative error of at most 0.0003.
Values sent between devices are 32-bit elements.
A program may use at most 64 MiB of HBM per device.

```python
import jax
import jax.numpy as jnp
from jax import lax

BLOCKS_DEV = 4
ROWS = 128
LANES = 128
BLOCKS = 64
LAYERS = 3
N_QA = 4
N_QB = 4


def block_scale(own_key, dims, pieces, smallest, high):
    def one(position, blocks):
        heights = jax.random.uniform(jax.random.fold_in(jax.random.fold_in(own_key, 6), position), (blocks,), jnp.float32, smallest / len(pieces), high / len(pieces))
        return jnp.repeat(jnp.exp(heights), dims[position] // blocks).reshape((-1,) + (1,) * (len(dims) - position - 1))

    factor_of = one(*pieces[0])
    for cut in pieces[1:]:
        factor_of = factor_of * one(*cut)
    return factor_of


def scatter_about(rng, dims, spread, most, cuts=(), kind=jnp.bfloat16):
    values = spread * jax.random.normal(rng, dims, jnp.float32)
    if cuts:
        values = values * block_scale(rng, dims, cuts, -0.22, 0.18)
    return jnp.clip(values, -most, most).astype(kind)


def setup_inputs(seed: int = 0, part: int = 0) -> dict:
    key_of = jax.random.split(jax.random.key(seed), 5)
    own_keys = jax.random.split(jax.random.fold_in(key_of[4], part), 5)
    wave_parts = scatter_about(own_keys[0], (2, BLOCKS, ROWS, LANES), 1.0, 6.0, ((1, 16),), jnp.float32)
    level_table = jnp.clip(jax.random.uniform(own_keys[1], (BLOCKS, ROWS, LANES), jnp.float32, -2.0, 2.0) * block_scale(own_keys[1], (BLOCKS, ROWS, LANES), ((0, 16),), -0.4, 0.0), -2.0, 2.0)
    diagonal_angles = jnp.clip(jax.random.uniform(own_keys[2], (LAYERS, LANES), jnp.float32, 0.3, 1.2), 0.3, 1.2)
    turn_angles = jnp.clip(jax.random.uniform(own_keys[3], (LAYERS, 4), jnp.float32, 0.3, 1.2), 0.3, 1.2)
    return dict(wave_parts=wave_parts, level_table=level_table, diagonal_angles=diagonal_angles, turn_angles=turn_angles)


def count_bits(values, count):
    places = jnp.arange(count.bit_length() - 1, dtype=jnp.int32)
    return jnp.sum((values[..., None] >> places) & 1, axis=-1)


def rotation_table(count, angle):
    rank = jnp.arange(count, dtype=jnp.int32)
    apart = count_bits(rank[:, None] ^ rank[None, :], count)
    bits = count.bit_length() - 1
    size = jnp.cos(angle) ** (bits - apart).astype(jnp.float32) * jnp.sin(angle) ** apart.astype(jnp.float32)
    real_sign = jnp.where(apart % 4 == 0, 1.0, jnp.where(apart % 4 == 2, -1.0, 0.0)).astype(jnp.float32)
    imag_sign = jnp.where(apart % 4 == 1, -1.0, jnp.where(apart % 4 == 3, 1.0, 0.0)).astype(jnp.float32)
    return size * real_sign, size * imag_sign


def mix_dim(values, dim, angle):
    real_part, imag_part = rotation_table(values.shape[dim], angle)
    def times(table):
        moved = jnp.tensordot(values, table, axes=([dim], [0]), precision=lax.Precision.HIGHEST)
        return jnp.moveaxis(moved, -1, dim)
    by_real = times(real_part)
    by_imag = times(imag_part)
    return jnp.stack([by_real[0] - by_imag[1], by_real[1] + by_imag[0]])


def phase_step(values, levels, angle):
    turn = angle * levels
    return jnp.stack([values[0] * jnp.cos(turn) + values[1] * jnp.sin(turn), values[1] * jnp.cos(turn) - values[0] * jnp.sin(turn)])


def reference(wave_parts, level_table, diagonal_angles, turn_angles):
    values = wave_parts
    for layer in range(LAYERS):
        values = phase_step(values, level_table, diagonal_angles[layer])
        values = mix_dim(values, 3, turn_angles[layer, 0])
        values = mix_dim(values, 2, turn_angles[layer, 1])
        parts = values.reshape(2, N_QA, N_QB, BLOCKS_DEV, ROWS, LANES)
        parts = mix_dim(parts, 1, turn_angles[layer, 2])
        parts = mix_dim(parts, 2, turn_angles[layer, 3])
        parts = mix_dim(parts, 3, turn_angles[layer, 2])
        values = parts.reshape(values.shape)
    return values
```

```python
import functools

import jax
import jax.numpy as jnp
from jax import lax
from jax.experimental import pallas as pl
from jax.experimental.pallas import tpu as pltpu
from jax.sharding import PartitionSpec as P

LAYERS = 3


def count_bits(values, count):
    places = jnp.arange(count.bit_length() - 1, dtype=jnp.int32)
    return jnp.sum(values[..., None] >> places & 1, axis=-1)


def rotation_table(count, angle):
    rank = jnp.arange(count, dtype=jnp.int32)
    apart = count_bits(rank[:, None] ^ rank[None, :], count)
    bits = count.bit_length() - 1
    size = jnp.cos(angle) ** (bits - apart).astype(jnp.float32) * jnp.sin(angle) ** apart.astype(
        jnp.float32
    )
    real_sign = jnp.where(apart % 4 == 0, 1.0, jnp.where(apart % 4 == 2, -1.0, 0.0)).astype(
        jnp.float32
    )
    imag_sign = jnp.where(apart % 4 == 1, -1.0, jnp.where(apart % 4 == 3, 1.0, 0.0)).astype(
        jnp.float32
    )
    return (size * real_sign, size * imag_sign)


def mix_dim(values, dim, angle):
    real_part, imag_part = rotation_table(values.shape[dim], angle)

    def times(table):
        moved = jnp.tensordot(values, table, axes=([dim], [0]), precision=lax.Precision.HIGHEST)
        return jnp.moveaxis(moved, -1, dim)

    by_real = times(real_part)
    by_imag = times(imag_part)
    return jnp.stack([by_real[0] - by_imag[1], by_real[1] + by_imag[0]])


def phase_step(values, levels, angle):
    turn = angle * levels
    return jnp.stack(
        [
            values[0] * jnp.cos(turn) + values[1] * jnp.sin(turn),
            values[1] * jnp.cos(turn) - values[0] * jnp.sin(turn),
        ]
    )


def cos_sin(turn):
    half = 0.5 * turn
    y = half * half
    sine = -1 / 39916800
    for term in (1 / 362880, -1 / 5040, 1 / 120, -1 / 6, 1.0):
        sine = sine * y + term
    sine = sine * half
    cosine = 1 / 479001600
    for term in (-1 / 3628800, 1 / 40320, -1 / 720, 1 / 24, -0.5, 1.0):
        cosine = cosine * y + term
    return 1.0 - 2.0 * sine * sine, 2.0 * sine * cosine


def split(x):
    high = x.astype(jnp.bfloat16)
    return high, (x - high.astype(jnp.float32)).astype(jnp.bfloat16)


def times(a, b):
    dot = functools.partial(jnp.dot, preferred_element_type=jnp.float32)
    return dot(a[0], b[0]) + (dot(a[0], b[1]) + dot(a[1], b[0]))


def moved_bits(fields, order):
    def places(names):
        at, low = {}, 0
        for name in reversed(names):
            at[name] = low
            low += fields[name][0]
        return at

    into, out = places(order[0]), places(order[1])
    return [
        (out[name] + i, into[name] + i, group)
        for name, (bits, group) in fields.items()
        for i in range(bits)
    ]


def turn_table(size, bits, angles, out_axis):
    out = lax.broadcasted_iota(jnp.int32, (size, size), out_axis)
    into = lax.broadcasted_iota(jnp.int32, (size, size), 1 - out_axis)
    table = None
    for out_at, in_at, group in bits:
        o = (out >> out_at) & 1
        i = (into >> in_at) & 1
        if group is None:
            factor = jnp.where(o == i, 1.0, 0.0)
        else:
            c, s = angles[group]
            factor = jnp.where(o == i, c, jnp.where(o > i, -s, s))
        table = factor if table is None else table * factor
    return table


def mix_list(xs, groups, angles):
    xs = list(xs)
    step = len(xs)
    for group in groups:
        c, s = angles[group]
        step //= 2
        for j in range(len(xs)):
            if not j & step:
                u, v = xs[j], xs[j + step]
                xs[j], xs[j + step] = c * u + s * v, c * v - s * u
    return xs


def log2(count):
    return count.bit_length() - 1


def kernel(na, nb, wave, level, diag, turns, out, x1, s1, r1, x2, s2, r2, x3, s3, r3,
           tb, tp, tc, cs, send_sem, recv_sem, own_sem):
    n = na * nb
    blocks, rows, lanes = wave.shape[1:]
    high = n // blocks
    rest = rows // high
    low = rest // n
    f32 = jnp.float32
    a = lax.axis_index("qa")
    b = lax.axis_index("qb")
    me = a * nb + b

    def where_is(k):
        peer = lax.rem(me + k, n)
        return peer, {"qa": lax.div(peer, nb), "qb": lax.rem(peer, nb)}

    barrier = pltpu.get_barrier_semaphore()

    def greet(k, carry):
        pl.semaphore_signal(barrier, inc=1, device_id=where_is(k)[1], device_id_type=pl.DeviceIdType.MESH)
        return carry

    lax.fori_loop(1, n, greet, 0)

    def remote(src, dst, which, k):
        peer, to = where_is(k)
        return pltpu.make_async_remote_copy(
            src_ref=src(peer), dst_ref=dst(me), send_sem=send_sem.at[which, k],
            recv_sem=recv_sem.at[which, k], device_id=to, device_id_type=pl.DeviceIdType.MESH)

    def send(src, dst, which):
        def one(k, carry):
            remote(src, dst, which, k).start()
            return carry

        lax.fori_loop(1, n, one, 0)
        pltpu.make_async_copy(src(me), dst(me), own_sem.at[which]).start()

    def arrive(src, dst, which):
        def one(k, carry):
            remote(src, dst, which, k).wait_recv()
            return carry

        lax.fori_loop(1, n, one, 0)
        pltpu.make_async_copy(src(me), dst(me), own_sem.at[which]).wait()

    def sent(src, dst, which):
        def one(k, carry):
            remote(src, dst, which, k).wait_send()
            return carry

        lax.fori_loop(1, n, one, 0)

    plans = []
    for p in range(2):
        plans.append((lambda i, p=p: s1.at[p, i], lambda i, p=p: r1.at[p, i], p))
    for p in range(2):
        plans.append((lambda i, p=p: s2.at[p, :, i], lambda i, p=p: r2.at[p, i], 2 + p))
    for p in range(2):
        plans.append((lambda i, p=p: s3.at[p, i], lambda i, p=p: r3.at[p, i], 4 + p))
    per = n // blocks
    table_b = (lambda i: level.at[i // per, pl.ds(pl.multiple_of((i % per) * rest, 8), rest)], lambda i: tb.at[i], 6)
    table_c = (lambda i: tp.at[:, i], lambda i: tc.at[i], 7)

    angles = []
    for layer in range(LAYERS):
        angles.append([cos_sin(jnp.full((1, lanes), turns[layer, g], f32)) for g in range(4)])
    lane_bits = [(i, i, 0) for i in range(log2(lanes))]

    row_at = lax.broadcasted_iota(jnp.int32, (rows, lanes), 0)
    lane_at = lax.broadcasted_iota(jnp.int32, (rows, lanes), 1)
    ones = jnp.zeros((rows, lanes), jnp.int32)
    for i in range(log2(rows)):
        ones = ones + ((row_at >> i) & 1)
    for i in range(log2(lanes)):
        ones = ones + ((lane_at >> i) & 1)
    for i in range(log2(n)):
        ones = ones + lax.rem(lax.div(me, 1 << i), 2)

    def power(block):
        q = (ones + block.bit_count()) & 3
        real = jnp.where(q == 0, 1.0, jnp.where(q == 2, -1.0, 0.0))
        imag = jnp.where(q == 1, -1.0, jnp.where(q == 3, 1.0, 0.0))
        return real, imag

    for g in range(blocks):
        c, s = cos_sin(diag[0:1, :] * level[g])
        re, im = wave[0, g], wave[1, g]
        re, im = re * c + im * s, im * c - re * s
        fr, fi = power(g)
        x1[0, g] = re * fr - im * fi
        x1[1, g] = im * fr + re * fi

    pl.semaphore_wait(barrier, n - 1)
    send(*table_b)

    def segment(layer, bits, take, put, plan):
        turn = angles[layer]
        right = split(turn_table(lanes, lane_bits, turn, 1))
        left = split(turn_table(rows, bits, turn, 0))
        for p in range(2):
            xs = [times(left, split(times(split(take(p, g)), right))) for g in range(blocks)]
            for g, x in enumerate(mix_list(xs, [2] * log2(blocks), turn)):
                put(p, g, x)
            send(*plan[p])

    def join(received, table, layer, groups, take, put, plan, count):
        def phase(j, carry):
            c, s = cos_sin(diag[layer + 1 : layer + 2, :] * take(table, j))
            cs[0, j] = c
            cs[1, j] = s
            return carry

        lax.fori_loop(0, count, phase, 0)
        arrive(*plan[0])
        arrive(*plan[1])

        def step(j, carry):
            re = mix_list(take(received.at[0], j), groups, angles[layer])
            im = mix_list(take(received.at[1], j), groups, angles[layer])
            for i in range(n):
                c, s = cs[0, j, i], cs[1, j, i]
                put(0, i, j, re[i] * c + im[i] * s)
                put(1, i, j, im[i] * c - re[i] * s)
            return carry

        lax.fori_loop(0, count, step, 0)

    def put1(p, g, x):
        s1[p, g * per : (g + 1) * per] = x.reshape(per, rest, lanes)

    segment(0, [(i, i, 1) for i in range(log2(rows))], lambda p, g: x1[p, g], put1, plans[0:2])

    arrive(*table_b)
    fields_b = dict(b=(log2(nb), 3), mid=(log2(n), 1), low=(log2(low), 1))
    orders_b = (("b", "mid", "low"), ("mid", "b", "low"))
    bits_b = moved_bits(fields_b, orders_b)
    place = turn_table(rows, [(o, i, None) for o, i, _ in bits_b], None, 0).astype(jnp.bfloat16)
    for g in range(na):
        x = tb[g * nb : (g + 1) * nb].reshape(rows, lanes)
        first = x.astype(jnp.bfloat16)
        x = x - first.astype(f32)
        second = x.astype(jnp.bfloat16)
        third = (x - second.astype(f32)).astype(jnp.bfloat16)
        first, second, third = [jnp.dot(place, y, preferred_element_type=f32) for y in (first, second, third)]
        tp[g] = ((first + second) + third).reshape(n, nb * low, lanes)
    send(*table_c)

    def take_b(ref, j):
        return ref[:, pl.ds(pl.multiple_of(j * 8, 8), 8), :]

    def put_b(p, i, j, x):
        x2[p, i, pl.ds(pl.multiple_of(j * 8, 8), 8), :] = x

    join(r1, tb, 0, [2] * log2(na) + [3] * log2(nb), take_b, put_b, plans[0:2], rest // 8)

    def put2(p, g, x):
        s2[p, g] = x.reshape(n, nb * low, lanes)

    segment(1, bits_b, lambda p, g: x2[p, g * nb : (g + 1) * nb].reshape(rows, lanes), put2, plans[2:4])

    arrive(*table_c)

    def put_c(p, i, j, x):
        x3[p, i, j] = x

    join(r2, tc, 1, [2] * log2(blocks) + [1] * log2(high), lambda ref, j: ref[:, j], put_c, plans[2:4], na)

    fields_c = dict(block=(log2(blocks), 2), high=(log2(high), 1), b=(log2(nb), 3), low=(log2(low), 1))
    bits_c = moved_bits(fields_c, (("block", "high", "b", "low"), ("b", "block", "high", "low")))

    def put3(p, g, x):
        s3[p, g * nb : (g + 1) * nb] = x.reshape(nb, blocks, high * low, lanes)

    segment(2, bits_c, lambda p, g: x3[p, :, g].reshape(rows, lanes), put3, plans[4:6])

    fields_a = dict(mid=(log2(n), 1), high=(log2(high), None), low=(log2(low), None))
    bits_a = moved_bits(fields_a, (("mid", "high", "low"), ("high", "mid", "low")))
    last = split(turn_table(rows, bits_a, angles[2], 0))
    arrive(*plans[4])
    arrive(*plans[5])
    for g in range(blocks):
        re, im = [times(last, split(r3[p, :, g].reshape(rows, lanes))) for p in range(2)]
        fr, fi = power(g)
        out[0, g] = re * fr + im * fi
        out[1, g] = im * fr - re * fi
    for plan in plans + [table_b, table_c]:
        sent(*plan)


def fits(na, nb, blocks, rows):
    n = na * nb
    if blocks != na or n % blocks or rows * blocks % (n * n):
        return False
    high = n // blocks
    low = rows // high // n
    return nb * low == 8 and high * low == 8


def fused(wave_parts, level_table, diagonal_angles, turn_angles, na, nb):
    n = na * nb
    _, blocks, rows, lanes = wave_parts.shape
    rest = rows * blocks // n
    f32 = jnp.float32
    V = pltpu.VMEM
    flat = V((2, n, rest, lanes), f32)
    tiles = V((2, n, na, 8, lanes), f32)
    vmem = pl.BlockSpec(memory_space=pltpu.VMEM)
    return pl.pallas_call(
        functools.partial(kernel, na, nb),
        out_shape=jax.ShapeDtypeStruct(wave_parts.shape, f32),
        in_specs=[vmem, vmem, vmem, pl.BlockSpec(memory_space=pltpu.SMEM)],
        out_specs=vmem,
        scratch_shapes=[
            V(wave_parts.shape, f32), flat, flat,
            flat, V((2, na, n, 8, lanes), f32), tiles,
            tiles, V((2, n, blocks, 8, lanes), f32), V((2, n, blocks, 8, lanes), f32),
            V((n, rest, lanes), f32), V((na, n, 8, lanes), f32), V((n, na, 8, lanes), f32),
            V((2, na, n, 8, lanes), f32),
            pltpu.SemaphoreType.DMA((8, n)), pltpu.SemaphoreType.DMA((8, n)), pltpu.SemaphoreType.DMA((8,)),
        ],
        compiler_params=pltpu.CompilerParams(
            collective_id=0, has_side_effects=True, vmem_limit_bytes=32 * 1024 * 1024),
    )(wave_parts, level_table, diagonal_angles, turn_angles)


def shards(wave_parts, level_table, diagonal_angles, turn_angles):
    values = wave_parts
    for layer in range(LAYERS):
        values = phase_step(values, level_table, diagonal_angles[layer])
        values = mix_dim(values, 3, turn_angles[layer, 0])
        values = mix_dim(values, 2, turn_angles[layer, 1])
        moved = lax.all_to_all(values, "qa", split_axis=2, concat_axis=1, tiled=True)
        moved = mix_dim(moved, 1, turn_angles[layer, 2])
        values = lax.all_to_all(moved, "qa", split_axis=1, concat_axis=2, tiled=True)
        moved = lax.all_to_all(values, "qb", split_axis=3, concat_axis=1, tiled=True)
        spread = moved.reshape(2, lax.axis_size("qb"), -1, moved.shape[2], moved.shape[3])
        moved = mix_dim(spread, 1, turn_angles[layer, 3]).reshape(moved.shape)
        values = lax.all_to_all(moved, "qb", split_axis=1, concat_axis=3, tiled=True)
    return values


def solution(mesh):
    na, nb = mesh.shape["qa"], mesh.shape["qb"]

    def each(wave_parts, level_table, diagonal_angles, turn_angles):
        args = (wave_parts, level_table, diagonal_angles, turn_angles)
        if fits(na, nb, wave_parts.shape[1], wave_parts.shape[2]):
            return fused(*args, na, nb)
        return shards(*args)

    placed = (
        P("trial", ("qa", "qb"), None, None),
        P(("trial", "qa", "qb"), None, None),
        P("trial", None),
        P("trial", None),
    )
    return jax.shard_map(
        each,
        mesh=mesh,
        in_specs=placed,
        out_specs=P("trial", ("qa", "qb"), None, None),
        check_vma=False,
    )
```

```python
import functools

import jax
import jax.numpy as jnp
from jax import lax
from jax.experimental import pallas as pl
from jax.experimental.pallas import tpu as pltpu
from jax.sharding import PartitionSpec as P

LAYERS = 3


def count_bits(values, count):
    places = jnp.arange(count.bit_length() - 1, dtype=jnp.int32)
    return jnp.sum(values[..., None] >> places & 1, axis=-1)


def rotation_table(count, angle):
    rank = jnp.arange(count, dtype=jnp.int32)
    apart = count_bits(rank[:, None] ^ rank[None, :], count)
    bits = count.bit_length() - 1
    size = jnp.cos(angle) ** (bits - apart).astype(jnp.float32) * jnp.sin(angle) ** apart.astype(
        jnp.float32
    )
    real_sign = jnp.where(apart % 4 == 0, 1.0, jnp.where(apart % 4 == 2, -1.0, 0.0)).astype(
        jnp.float32
    )
    imag_sign = jnp.where(apart % 4 == 1, -1.0, jnp.where(apart % 4 == 3, 1.0, 0.0)).astype(
        jnp.float32
    )
    return (size * real_sign, size * imag_sign)


def mix_dim(values, dim, angle):
    real_part, imag_part = rotation_table(values.shape[dim], angle)

    def times(table):
        moved = jnp.tensordot(values, table, axes=([dim], [0]), precision=lax.Precision.HIGHEST)
        return jnp.moveaxis(moved, -1, dim)

    by_real = times(real_part)
    by_imag = times(imag_part)
    return jnp.stack([by_real[0] - by_imag[1], by_real[1] + by_imag[0]])


def phase_step(values, levels, angle):
    turn = angle * levels
    return jnp.stack(
        [
            values[0] * jnp.cos(turn) + values[1] * jnp.sin(turn),
            values[1] * jnp.cos(turn) - values[0] * jnp.sin(turn),
        ]
    )


def cos_sin(turn):
    half = 0.5 * turn
    y = half * half
    sine = -1 / 39916800
    for term in (1 / 362880, -1 / 5040, 1 / 120, -1 / 6, 1.0):
        sine = sine * y + term
    sine = sine * half
    cosine = 1 / 479001600
    for term in (-1 / 3628800, 1 / 40320, -1 / 720, 1 / 24, -0.5, 1.0):
        cosine = cosine * y + term
    return 1.0 - 2.0 * sine * sine, 2.0 * sine * cosine


def split(x):
    high = x.astype(jnp.bfloat16)
    return high, (x - high.astype(jnp.float32)).astype(jnp.bfloat16)


def times(a, b):
    dot = functools.partial(jnp.dot, preferred_element_type=jnp.float32)
    return dot(a[0], b[0]) + (dot(a[0], b[1]) + dot(a[1], b[0]))


def moved_bits(fields, order):
    def places(names):
        at, low = {}, 0
        for name in reversed(names):
            at[name] = low
            low += fields[name][0]
        return at

    into, out = places(order[0]), places(order[1])
    return [
        (out[name] + i, into[name] + i, group)
        for name, (bits, group) in fields.items()
        for i in range(bits)
    ]


def turn_table(size, bits, angles, out_axis):
    out = lax.broadcasted_iota(jnp.int32, (size, size), out_axis)
    into = lax.broadcasted_iota(jnp.int32, (size, size), 1 - out_axis)
    table = None
    for out_at, in_at, group in bits:
        o = (out >> out_at) & 1
        i = (into >> in_at) & 1
        if group is None:
            factor = jnp.where(o == i, 1.0, 0.0)
        else:
            c, s = angles[group]
            factor = jnp.where(o == i, c, jnp.where(o > i, -s, s))
        table = factor if table is None else table * factor
    return table


def mix_list(xs, groups, angles):
    xs = list(xs)
    step = len(xs)
    for group in groups:
        c, s = angles[group]
        step //= 2
        for j in range(len(xs)):
            if not j & step:
                u, v = xs[j], xs[j + step]
                xs[j], xs[j + step] = c * u + s * v, c * v - s * u
    return xs


def log2(count):
    return count.bit_length() - 1


def kernel(na, nb, wave, level, diag, turns, out, x1, s1, r1, x2, s2, r2, x3, s3, r3,
           tb, tp, tc, cs, send_sem, recv_sem, own_sem):
    n = na * nb
    blocks, rows, lanes = wave.shape[1:]
    high = n // blocks
    rest = rows // high
    low = rest // n
    f32 = jnp.float32
    a = lax.axis_index("qa")
    b = lax.axis_index("qb")
    me = a * nb + b

    def flipped(x, mask):
        for i in range(log2(n)):
            if mask >> i & 1:
                x = x + (1 << i) * (1 - 2 * lax.rem(lax.div(x, 1 << i), 2))
        return x

    def where_is(k):
        pa, pb = flipped(a, k // nb), flipped(b, k % nb)
        return pa * nb + pb, {"qa": pa, "qb": pb}

    masks = sorted(range(1, n), key=lambda k: (-(k % nb), -(k // nb)))

    barrier = pltpu.get_barrier_semaphore()

    for k in masks:
        pl.semaphore_signal(barrier, inc=1, device_id=where_is(k)[1], device_id_type=pl.DeviceIdType.MESH)

    def remote(src, dst, which, k):
        peer, to = where_is(k)
        return pltpu.make_async_remote_copy(
            src_ref=src(peer), dst_ref=dst(me), send_sem=send_sem.at[which, k],
            recv_sem=recv_sem.at[which, k], device_id=to, device_id_type=pl.DeviceIdType.MESH)

    def send(src, dst, which):
        for k in masks:
            remote(src, dst, which, k).start()
        pltpu.make_async_copy(src(me), dst(me), own_sem.at[which]).start()

    def arrive(src, dst, which):
        for k in masks:
            remote(src, dst, which, k).wait_recv()
        pltpu.make_async_copy(src(me), dst(me), own_sem.at[which]).wait()

    def sent(src, dst, which):
        for k in masks:
            remote(src, dst, which, k).wait_send()

    plans = []
    for p in range(2):
        plans.append((lambda i, p=p: s1.at[p, i], lambda i, p=p: r1.at[p, i], p))
    for p in range(2):
        plans.append((lambda i, p=p: s2.at[p, :, i], lambda i, p=p: r2.at[p, i], 2 + p))
    for p in range(2):
        plans.append((lambda i, p=p: s3.at[p, i], lambda i, p=p: r3.at[p, i], 4 + p))
    per = n // blocks
    table_b = (lambda i: level.at[i // per, pl.ds(pl.multiple_of((i % per) * rest, 8), rest)], lambda i: tb.at[i], 6)
    table_c = (lambda i: tp.at[:, i], lambda i: tc.at[i], 7)

    angles = []
    for layer in range(LAYERS):
        angles.append([cos_sin(jnp.full((1, lanes), turns[layer, g], f32)) for g in range(4)])
    lane_bits = [(i, i, 0) for i in range(log2(lanes))]

    row_at = lax.broadcasted_iota(jnp.int32, (rows, lanes), 0)
    lane_at = lax.broadcasted_iota(jnp.int32, (rows, lanes), 1)
    ones = jnp.zeros((rows, lanes), jnp.int32)
    for i in range(log2(rows)):
        ones = ones + ((row_at >> i) & 1)
    for i in range(log2(lanes)):
        ones = ones + ((lane_at >> i) & 1)
    for i in range(log2(n)):
        ones = ones + lax.rem(lax.div(me, 1 << i), 2)

    def power(block):
        q = (ones + block.bit_count()) & 3
        real = jnp.where(q == 0, 1.0, jnp.where(q == 2, -1.0, 0.0))
        imag = jnp.where(q == 1, -1.0, jnp.where(q == 3, 1.0, 0.0))
        return real, imag

    pl.semaphore_wait(barrier, n - 1)
    send(*table_b)

    for g in range(blocks):
        c, s = cos_sin(diag[0:1, :] * level[g])
        re, im = wave[0, g], wave[1, g]
        re, im = re * c + im * s, im * c - re * s
        fr, fi = power(g)
        x1[0, g] = re * fr - im * fi
        x1[1, g] = im * fr + re * fi

    def segment(layer, bits, take, put, plan):
        turn = angles[layer]
        right = split(turn_table(lanes, lane_bits, turn, 1))
        left = split(turn_table(rows, bits, turn, 0))
        for p in range(2):
            xs = [times(left, split(times(split(take(p, g)), right))) for g in range(blocks)]
            for g, x in enumerate(mix_list(xs, [2] * log2(blocks), turn)):
                put(p, g, x)
            send(*plan[p])

    def join(received, table, layer, groups, take, put, plan, count):
        def phase(j, carry):
            c, s = cos_sin(diag[layer + 1 : layer + 2, :] * take(table, j))
            cs[0, j] = c
            cs[1, j] = s
            return carry

        lax.fori_loop(0, count, phase, 0)
        arrive(*plan[0])
        if layer == 0:
            send(*table_c)
        arrive(*plan[1])

        def step(j, carry):
            re = mix_list(take(received.at[0], j), groups, angles[layer])
            im = mix_list(take(received.at[1], j), groups, angles[layer])
            for i in range(n):
                c, s = cs[0, j, i], cs[1, j, i]
                put(0, i, j, re[i] * c + im[i] * s)
                put(1, i, j, im[i] * c - re[i] * s)
            return carry

        lax.fori_loop(0, count, step, 0)

    def put1(p, g, x):
        s1[p, g * per : (g + 1) * per] = x.reshape(per, rest, lanes)

    segment(0, [(i, i, 1) for i in range(log2(rows))], lambda p, g: x1[p, g], put1, plans[0:2])

    arrive(*table_b)
    fields_b = dict(b=(log2(nb), 3), mid=(log2(n), 1), low=(log2(low), 1))
    orders_b = (("b", "mid", "low"), ("mid", "b", "low"))
    bits_b = moved_bits(fields_b, orders_b)
    place = turn_table(rows, [(o, i, None) for o, i, _ in bits_b], None, 0).astype(jnp.bfloat16)
    for g in range(na):
        x = tb[g * nb : (g + 1) * nb].reshape(rows, lanes)
        first = x.astype(jnp.bfloat16)
        x = x - first.astype(f32)
        second = x.astype(jnp.bfloat16)
        third = (x - second.astype(f32)).astype(jnp.bfloat16)
        first, second, third = [jnp.dot(place, y, preferred_element_type=f32) for y in (first, second, third)]
        tp[g] = ((first + second) + third).reshape(n, nb * low, lanes)
    def take_b(ref, j):
        return ref[:, pl.ds(pl.multiple_of(j * 8, 8), 8), :]

    def put_b(p, i, j, x):
        x2[p, i, pl.ds(pl.multiple_of(j * 8, 8), 8), :] = x

    join(r1, tb, 0, [2] * log2(na) + [3] * log2(nb), take_b, put_b, plans[0:2], rest // 8)

    def put2(p, g, x):
        s2[p, g] = x.reshape(n, nb * low, lanes)

    segment(1, bits_b, lambda p, g: x2[p, g * nb : (g + 1) * nb].reshape(rows, lanes), put2, plans[2:4])

    arrive(*table_c)

    def put_c(p, i, j, x):
        x3[p, i, j] = x

    join(r2, tc, 1, [2] * log2(blocks) + [1] * log2(high), lambda ref, j: ref[:, j], put_c, plans[2:4], na)

    fields_c = dict(block=(log2(blocks), 2), high=(log2(high), 1), b=(log2(nb), 3), low=(log2(low), 1))
    bits_c = moved_bits(fields_c, (("block", "high", "b", "low"), ("b", "block", "high", "low")))

    def put3(p, g, x):
        s3[p, g * nb : (g + 1) * nb] = x.reshape(nb, blocks, high * low, lanes)

    segment(2, bits_c, lambda p, g: x3[p, :, g].reshape(rows, lanes), put3, plans[4:6])

    fields_a = dict(mid=(log2(n), 1), high=(log2(high), None), low=(log2(low), None))
    bits_a = moved_bits(fields_a, (("mid", "high", "low"), ("high", "mid", "low")))
    last = split(turn_table(rows, bits_a, angles[2], 0))
    arrive(*plans[4])
    arrive(*plans[5])
    for g in range(blocks):
        re, im = [times(last, split(r3[p, :, g].reshape(rows, lanes))) for p in range(2)]
        fr, fi = power(g)
        out[0, g] = re * fr + im * fi
        out[1, g] = im * fr - re * fi
    for plan in plans + [table_b, table_c]:
        sent(*plan)


def fits(na, nb, blocks, rows):
    n = na * nb
    if blocks != na or n % blocks or rows * blocks % (n * n):
        return False
    high = n // blocks
    low = rows // high // n
    return nb * low == 8 and high * low == 8


def fused(wave_parts, level_table, diagonal_angles, turn_angles, na, nb):
    n = na * nb
    _, blocks, rows, lanes = wave_parts.shape
    rest = rows * blocks // n
    f32 = jnp.float32
    V = pltpu.VMEM
    flat = V((2, n, rest, lanes), f32)
    tiles = V((2, n, na, 8, lanes), f32)
    vmem = pl.BlockSpec(memory_space=pltpu.VMEM)
    return pl.pallas_call(
        functools.partial(kernel, na, nb),
        out_shape=jax.ShapeDtypeStruct(wave_parts.shape, f32),
        in_specs=[vmem, vmem, vmem, pl.BlockSpec(memory_space=pltpu.SMEM)],
        out_specs=vmem,
        scratch_shapes=[
            V(wave_parts.shape, f32), flat, flat,
            flat, V((2, na, n, 8, lanes), f32), tiles,
            tiles, V((2, n, blocks, 8, lanes), f32), V((2, n, blocks, 8, lanes), f32),
            V((n, rest, lanes), f32), V((na, n, 8, lanes), f32), V((n, na, 8, lanes), f32),
            V((2, na, n, 8, lanes), f32),
            pltpu.SemaphoreType.DMA((8, n)), pltpu.SemaphoreType.DMA((8, n)), pltpu.SemaphoreType.DMA((8,)),
        ],
        compiler_params=pltpu.CompilerParams(
            collective_id=0, has_side_effects=True, vmem_limit_bytes=32 * 1024 * 1024),
    )(wave_parts, level_table, diagonal_angles, turn_angles)


def shards(wave_parts, level_table, diagonal_angles, turn_angles):
    values = wave_parts
    for layer in range(LAYERS):
        values = phase_step(values, level_table, diagonal_angles[layer])
        values = mix_dim(values, 3, turn_angles[layer, 0])
        values = mix_dim(values, 2, turn_angles[layer, 1])
        moved = lax.all_to_all(values, "qa", split_axis=2, concat_axis=1, tiled=True)
        moved = mix_dim(moved, 1, turn_angles[layer, 2])
        values = lax.all_to_all(moved, "qa", split_axis=1, concat_axis=2, tiled=True)
        moved = lax.all_to_all(values, "qb", split_axis=3, concat_axis=1, tiled=True)
        spread = moved.reshape(2, lax.axis_size("qb"), -1, moved.shape[2], moved.shape[3])
        moved = mix_dim(spread, 1, turn_angles[layer, 3]).reshape(moved.shape)
        values = lax.all_to_all(moved, "qb", split_axis=1, concat_axis=3, tiled=True)
    return values


def solution(mesh):
    na, nb = mesh.shape["qa"], mesh.shape["qb"]

    def each(wave_parts, level_table, diagonal_angles, turn_angles):
        args = (wave_parts, level_table, diagonal_angles, turn_angles)
        if fits(na, nb, wave_parts.shape[1], wave_parts.shape[2]):
            return fused(*args, na, nb)
        return shards(*args)

    placed = (
        P("trial", ("qa", "qb"), None, None),
        P(("trial", "qa", "qb"), None, None),
        P("trial", None),
        P("trial", None),
    )
    return jax.shard_map(
        each,
        mesh=mesh,
        in_specs=placed,
        out_specs=P("trial", ("qa", "qb"), None, None),
        check_vma=False,
    )
```
